32 devices in a mesh: section: 8 (over z, y), fsdp: 4 (over x, core).
Axes of the slice: x: 2, y: 2, z: 4, core: 2. Of those that a mesh axis runs over, the one named last changes fastest.
Arguments:
- source_rows: bfloat16 [3072, 4096], P(('section', 'fsdp')), may hold values from -6 to 6
- target_rows: bfloat16 [1024, 4096], P('section'), may hold values from -6 to 6
- attn_weights: bfloat16 [8, 4, 4096, 3072], P('section', None, None, 'fsdp'), may hold values from -3.76875 to 3.76875
- gains: float32 [8, 4096], P('section'), may hold values from 0.25 to 1.75
- lengths: int32 [8], P('section'), may hold values from 192 to 384
Outputs:
- source_next: bfloat16 [3072, 4096], P(('section', 'fsdp'))
- target_next: bfloat16 [1024, 4096], P('section')
The draws below stay inside these ranges and needn't reach their ends.
Inputs may be any that keep to these rules, and one draw needn't show every extreme that they name: Keys at positions lengths[s] and beyond are padding.
All inputs are finite; a program needn't handle non-finite values.
Results may differ from the reference program's by a relative error of at most 0.015.
The reference program's roundings to bfloat16 on the way count: a program that leaves them out, or rounds other values in their place, can miss the bound.
Values may be sent and summed in bfloat16 or wider, within the bound.
A program may use at most 128 MiB of HBM per device.

```python
import math
import jax
import jax.numpy as jnp
from jax import lax

D = 4096
HEAD_DIM = 64
IN_LEN = 384
OUT_LEN = 128
INNER = 3072
SOURCE_TOTAL = 3072
TARGET_TOTAL = 1024
N_SECTION = 8
N_FSDP = 4


def draw_attn_weights(key, part):
    shape_all = (N_SECTION, 4, D, INNER)
    drawn = jnp.clip(jax.random.normal(key, shape_all, jnp.float32), -6.0, 6.0) / math.sqrt(D)
    return drawn.astype(jnp.bfloat16)


def touch_ends(array, stream_key, least, high):
    longest = array.shape.index(max(array.shape))
    spots = []
    for shift in (0, 1):
        where = [jax.random.randint(jax.random.fold_in(stream_key, axis), (), 0, length) for axis, length in enumerate(array.shape)]
        where[longest] = (where[longest] + shift) % array.shape[longest]
        spots.append(tuple(where))
    return array.at[spots[0]].set(least).at[spots[1]].set(high)


def block_levels(rng, extent, shards, smallest, high):
    gain, own = 1.0, jax.random.fold_in(rng, 6)
    for position, parts in shards:
        draws = jnp.exp(jax.random.uniform(jax.random.fold_in(own, position), (parts,), jnp.float32, smallest / len(shards), high / len(shards)))
        gain = gain * jnp.repeat(draws, extent[position] // parts).reshape([-1 if axis == position else 1 for axis in range(len(extent))])
    return gain


def centred(stream_key, shape, deviation, limit, split=(), kind=jnp.bfloat16):
    result = deviation * jax.random.normal(stream_key, shape, jnp.float32)
    if split:
        result = result * block_levels(stream_key, shape, split, -0.22, 0.18)
    return jnp.clip(result, -limit, limit).astype(kind)


def setup_inputs(seed: int = 0) -> dict:
    keys = jax.random.split(jax.random.key(seed), 6)
    source_rows = centred(keys[0], (SOURCE_TOTAL, D), 1.0, 6.0, ((0, 32),))
    target_rows = centred(keys[1], (TARGET_TOTAL, D), 1.0, 6.0, ((0, 8),))
    attn_weights = draw_attn_weights(jax.random.fold_in(keys[5], 71), 0)
    gains = jnp.clip(1.0 + 0.15 * jax.random.normal(keys[3], (N_SECTION, D), jnp.float32), 0.25, 1.75)
    lengths = touch_ends(jax.random.randint(keys[4], (N_SECTION,), IN_LEN // 2, IN_LEN + 1), jax.random.fold_in(keys[4], 1), IN_LEN // 2, IN_LEN).astype(jnp.int32)
    return dict(source_rows=source_rows, target_rows=target_rows, attn_weights=attn_weights, gains=gains, lengths=lengths)


def rms_norm(block_rows, gain_row):
    widened = block_rows.astype(jnp.float32)
    inverse_rms = lax.rsqrt(lax.optimization_barrier(jnp.mean(widened * widened, axis=-1, keepdims=True)) + 1e-06)
    return (widened * inverse_rms * gain_row).astype(jnp.bfloat16)

def project(block_rows, weight):
    return jnp.dot(block_rows, weight, preferred_element_type=jnp.float32).astype(jnp.bfloat16)

def attend(queries, key_rows, values, length):
    query_count = queries.shape[0]
    key_count = key_rows.shape[0]
    head_count = queries.shape[1] // HEAD_DIM
    query_heads = queries.reshape(query_count, head_count, HEAD_DIM).astype(jnp.float32)
    key_heads = key_rows.reshape(key_count, head_count, HEAD_DIM).astype(jnp.float32)
    value_heads = values.reshape(key_count, head_count, HEAD_DIM).astype(jnp.float32)
    scores = jnp.einsum('qhc,khc->hqk', query_heads, key_heads) * 0.125
    key_valid = jnp.arange(key_count, dtype=jnp.int32) < length
    scores = jnp.where(key_valid[None, None, :], scores, -1000000000.0)
    row_max = lax.optimization_barrier(jnp.max(scores, axis=-1, keepdims=True))
    expo = jnp.exp(scores - row_max)
    soft = (expo / lax.optimization_barrier(jnp.sum(expo, axis=-1, keepdims=True))).astype(jnp.bfloat16)
    context = jnp.einsum('hqk,khc->qhc', soft.astype(jnp.float32), value_heads)
    return context.reshape(query_count, head_count * HEAD_DIM).astype(jnp.bfloat16)

def out_terms(context, out_weight):
    row_count = context.shape[0]
    context_groups = context.reshape(row_count, N_FSDP, -1).astype(jnp.float32)
    weight_groups = out_weight.reshape(out_weight.shape[0], N_FSDP, -1).astype(jnp.float32)
    group_terms = jnp.einsum('rgc,dgc->grd', context_groups, weight_groups)
    rounded = lax.optimization_barrier(group_terms.astype(jnp.bfloat16))
    return lax.optimization_barrier(jnp.sum(rounded.astype(jnp.float32), axis=0))

def reference(source_rows, target_rows, attn_weights, gains, lengths):
    half_sections = N_SECTION // 2
    source_blocks = source_rows.reshape(N_SECTION, IN_LEN, D)
    target_blocks = target_rows.reshape(N_SECTION, OUT_LEN, D)
    source_out = []
    target_out = []
    for section_index in range(N_SECTION):
        weights = attn_weights[section_index]
        gain_row = gains[section_index]
        length = lengths[section_index]
        source_block = source_blocks[section_index]
        target_block = target_blocks[section_index]
        if section_index < half_sections:
            normed = rms_norm(source_block, gain_row)
            context = attend(project(normed, weights[0]), project(normed, weights[1]), project(normed, weights[2]), length)
            source_block = (source_block.astype(jnp.float32) + out_terms(context, weights[3])).astype(jnp.bfloat16)
        else:
            normed = rms_norm(target_block, gain_row)
            context = attend(project(normed, weights[0]), project(source_block, weights[1]), project(source_block, weights[2]), length)
            target_block = (target_block.astype(jnp.float32) + out_terms(context, weights[3])).astype(jnp.bfloat16)
        source_out.append(source_block)
        target_out.append(target_block)
    source_next = jnp.roll(jnp.stack(source_out), 1, axis=0).reshape(N_SECTION * IN_LEN, D)
    target_next = jnp.roll(jnp.stack(target_out), 1, axis=0).reshape(N_SECTION * OUT_LEN, D)
    return (source_next, target_next)
```

```python
import functools

import jax
import jax.numpy as jnp
from jax import lax
from jax.experimental import pallas as pl
from jax.experimental.pallas import tpu as pltpu
from jax.sharding import PartitionSpec as P

HEAD_DIM = 64
PIECES = 4
F32 = jnp.float32
BF16 = jnp.bfloat16


def row_chunks(rows):
    return 3 if rows % 48 == 0 else 1


def rms_norm(block, gain):
    wide = block.astype(F32)
    inverse = lax.rsqrt(jnp.mean(wide * wide, axis=-1, keepdims=True) + 1e-06)
    return (wide * inverse * gain).astype(BF16)


def kernel(
    n_sec, n_f, x_ref, y_ref, gain_ref, len_ref, w_hbm, so_hbm, to_hbm,
    xs, nb, ny, w, qkv, ctx, term, prt, sums, rem, own, prt_own, fin, sland,
    dterm, dprt, dp, yfin, tland,
    w_sem, l_sem, ag_s, ag_r, pt_s, pt_r, fw_s, fw_r, t1_s, t1_r, x1_s, x1_r,
    t2_s, t2_r, d1_s, d1_r, d2_s, d2_r, ss_s, ss_r, ts_s, ts_r, tf_s, tf_r, o_sem,
):
    chips = n_f // 2
    rows, d = x_ref.shape
    pair = 2 * rows
    total = pair * chips
    t_rows = y_ref.shape[0]
    t_half = t_rows // 2
    width = w.shape[2]
    chunks = row_chunks(rows)
    rc = rows // chunks
    cn = d // PIECES
    sec, f = lax.axis_index("section"), lax.axis_index("fsdp")
    core, chip = lax.rem(f, 2), f // 2
    other = 1 - core
    enc = sec < n_sec // 2
    partner = {"fsdp": chip * 2 + other}
    nxt = {"section": lax.rem(sec + 1, n_sec)}
    prv = {"section": lax.rem(sec + n_sec - 1, n_sec)}

    def ahead(k):
        return lax.rem(chip + k, chips)

    def behind(k):
        return lax.rem(chip + chips - k, chips)

    def peer(h):
        return {"fsdp": h * 2 + core}

    def remote(src, dst, send, recv, dev):
        return pltpu.make_async_remote_copy(
            src_ref=src, dst_ref=dst, send_sem=send, recv_sem=recv,
            device_id=dev, device_id_type=pl.DeviceIdType.MESH,
        )

    def at(start, size):
        return pl.ds(pl.multiple_of(start, 16), size)

    def cols(j):
        return pl.ds(j * cn, cn)

    barrier = pltpu.get_barrier_semaphore()
    greet = [partner, nxt, prv] + [peer(ahead(k)) for k in range(1, chips)]
    for dev in greet:
        pl.semaphore_signal(barrier, inc=1, device_id=dev, device_id_type=pl.DeviceIdType.MESH)

    w_copies = [pltpu.make_async_copy(w_hbm.at[0, i], w.at[i], w_sem.at[i]) for i in range(4)]
    for cp in w_copies:
        cp.start()
    home = pltpu.make_async_copy(x_ref, xs.at[at(f * rows, rows), :], l_sem)
    home.start()
    pl.semaphore_wait(barrier, len(greet))

    def gather_send(k, i):
        return remote(
            x_ref.at[pl.ds(i * rc, rc), :], xs.at[at(f * rows + i * rc, rc), :],
            ag_s.at[k - 1, i], ag_r.at[k - 1, i], peer(ahead(k)),
        )

    def gather_recv(k, i):
        spot = xs.at[at((behind(k) * 2 + core) * rows + i * rc, rc), :]
        return remote(spot, spot, ag_s.at[k - 1, i], ag_r.at[k - 1, i], peer(behind(k)))

    def forward(k, i, which):
        spot = xs.at[at((behind(k) * 2 + which) * rows + i * rc, rc), :]
        return remote(spot, spot, fw_s.at[k - 1, i], fw_r.at[k - 1, i], partner)

    own_rows = xs.at[at(f * rows, rows), :]
    mate_rows = xs.at[at((chip * 2 + other) * rows, rows), :]
    to_partner = remote(x_ref, own_rows, pt_s, pt_r, partner)
    to_partner.start()
    for i in range(chunks):
        for k in range(1, chips):
            gather_send(k, i).start()

    def shift_source(j, src):
        return remote(src.at[:, cols(j)], sland.at[:, cols(j)], ss_s.at[j], ss_r.at[j], nxt)

    def half(which):
        return at(which * t_half, t_half)

    def shift_target(j, src):
        return remote(src, tland.at[half(core), cols(j)], ts_s.at[j], ts_r.at[j], nxt)

    @pl.when(enc)
    def _():
        for j in range(PIECES):
            shift_target(j, y_ref.at[half(core), cols(j)]).start()

    @pl.when(jnp.logical_not(enc))
    def _():
        for j in range(PIECES):
            shift_source(j, x_ref).start()

    gain = gain_ref[...]
    tn = min(width, 256)

    def norm_rows(src, src_start, dst, dst_start, count):
        def step(r, carry):
            dst[at(dst_start + r * 16, 16), :] = rms_norm(src[at(src_start + r * 16, 16), :], gain)
            return carry

        lax.fori_loop(0, count // 16, step, 0)

    def prepare(src_start, dst_start, count):
        @pl.when(enc)
        def _():
            norm_rows(xs, src_start, nb, dst_start, count)

        @pl.when(jnp.logical_not(enc))
        def _():
            def step(r, carry):
                nb[at(dst_start + r * 16, 16), :] = xs[at(src_start + r * 16, 16), :]
                return carry

            lax.fori_loop(0, count // 16, step, 0)

    def project(src, which, start, count):
        def step(t, carry):
            lanes = pl.ds(pl.multiple_of(t * tn, 128), tn)
            qkv[which, at(start, count), lanes] = jnp.dot(
                src[...], w[which, :, lanes], preferred_element_type=F32
            ).astype(BF16)
            return carry

        lax.fori_loop(0, width // tn, step, 0)

    @pl.when(jnp.logical_not(enc))
    def _():
        norm_rows(y_ref, 0, ny, 0, t_rows)

    w_copies[0].wait()

    @pl.when(jnp.logical_not(enc))
    def _():
        project(ny, 0, 0, t_rows)

    for k in range(chips):
        h = behind(k)
        if k == 0:
            home.wait()
            prepare(f * rows, core * rows, rows)
            remote(mate_rows, mate_rows, pt_s, pt_r, partner).wait_recv()
            prepare((chip * 2 + other) * rows, other * rows, rows)
        else:
            for i in range(chunks):
                gather_recv(k, i).wait_recv()
                forward(k, i, core).start()
                prepare((h * 2 + core) * rows + i * rc, core * rows + i * rc, rc)
                forward(k, i, other).wait_recv()
                prepare((h * 2 + other) * rows + i * rc, other * rows + i * rc, rc)

        @pl.when(enc)
        def _():
            project(nb, 0, h * pair, pair)

        for which in (1, 2):
            if k == 0:
                w_copies[which].wait()
            project(nb, which, h * pair, pair)

    length = len_ref[0]

    def attend(start, count):
        key_ok = lax.broadcasted_iota(jnp.int32, (1, total), 1) < length
        first = lax.broadcasted_iota(jnp.int32, (1, 2 * HEAD_DIM), 1) < HEAD_DIM

        def step(t, carry):
            lanes = pl.ds(pl.multiple_of(t * 2 * HEAD_DIM, 128), 2 * HEAD_DIM)
            queries = qkv[0, at(start, count), lanes]
            keys, values = qkv[1, :, lanes], qkv[2, :, lanes]
            outs = []
            for low in (True, False):
                pick = first if low else jnp.logical_not(first)
                masked = queries * jnp.where(pick, 0.125, 0.0).astype(BF16)
                scores = lax.dot_general(
                    masked, keys, (((1,), (1,)), ((), ())), preferred_element_type=F32
                )
                scores = jnp.where(key_ok, scores, -1000000000.0)
                expo = jnp.exp(scores - jnp.max(scores, axis=-1, keepdims=True))
                soft = (expo * (1.0 / jnp.sum(expo, axis=-1, keepdims=True))).astype(BF16)
                outs.append(jnp.dot(soft, values, preferred_element_type=F32))
            ctx[at(start, count), lanes] = jnp.where(first, outs[0], outs[1]).astype(BF16)
            return carry

        lax.fori_loop(0, width // (2 * HEAD_DIM), step, 0)

    on = min(cn, 256)

    def out_piece(start, count, dst, j):
        def step(t, carry):
            lanes = pl.ds(pl.multiple_of(j * cn + t * on, 128), on)
            dst[:, lanes] = lax.dot_general(
                ctx[at(start, count), :], w[3, lanes, :], (((1,), (1,)), ((), ())),
                preferred_element_type=F32,
            ).astype(BF16)
            return carry

        lax.fori_loop(0, cn // on, step, 0)

    def mate_term(k, j):
        return remote(
            term.at[k - 1, at(other * rows, rows), cols(j)], prt.at[k - 1, :, cols(j)],
            t1_s.at[k - 1, j], t1_r.at[k - 1, j], partner,
        )

    def send_sum(k, j):
        return remote(
            sums.at[k - 1, :, cols(j)], rem.at[k - 1, :, cols(j)],
            x1_s.at[k - 1, j], x1_r.at[k - 1, j], peer(ahead(k)),
        )

    def mate_own(j):
        return remote(
            own.at[at(other * rows, rows), cols(j)], prt_own.at[:, cols(j)],
            t2_s.at[j], t2_r.at[j], partner,
        )

    def mate_target(j):
        return remote(
            dterm.at[half(other), cols(j)], dprt.at[:, cols(j)], d1_s.at[j], d1_r.at[j], partner
        )

    def send_target(k, j):
        return remote(
            dp.at[chip, :, cols(j)], dp.at[chip, :, cols(j)],
            d2_s.at[k - 1, j], d2_r.at[k - 1, j], peer(ahead(k)),
        )

    def recv_target(k, j):
        spot = dp.at[behind(k), :, cols(j)]
        return remote(spot, spot, d2_s.at[k - 1, j], d2_r.at[k - 1, j], peer(behind(k)))

    w_copies[3].wait()

    @pl.when(enc)
    def _():
        for k in range(1, chips):
            start = ahead(k) * pair
            attend(start, pair)

            def pass_on(j):
                mate_term(k, j).wait_recv()
                mine = term[k - 1, at(core * rows, rows), cols(j)].astype(F32)
                sums[k - 1, :, cols(j)] = (mine + prt[k - 1, :, cols(j)].astype(F32)).astype(BF16)
                send_sum(k, j).start()

            for j in range(PIECES):
                out_piece(start, pair, term.at[k - 1], j)
                mate_term(k, j).start()
                if j:
                    pass_on(j - 1)
            pass_on(PIECES - 1)
        attend(chip * pair, pair)
        for j in range(PIECES):
            out_piece(chip * pair, pair, own, j)
            mate_own(j).start()
        for j in range(PIECES):
            mate_own(j).wait_recv()
            delta = own[at(core * rows, rows), cols(j)].astype(F32) + prt_own[:, cols(j)].astype(F32)
            for k in range(1, chips):
                send_sum(k, j).wait_recv()
                delta += rem[k - 1, :, cols(j)].astype(F32)
            fin[:, cols(j)] = (x_ref[:, cols(j)].astype(F32) + delta).astype(BF16)
            shift_source(j, fin).start()
        for j in range(PIECES):
            mate_own(j).wait_send()
            for k in range(1, chips):
                mate_term(k, j).wait_send()
                send_sum(k, j).wait_send()

    @pl.when(jnp.logical_not(enc))
    def _():
        attend(0, t_rows)

        def pass_on(j):
            mate_target(j).wait_recv()
            mine = dterm[half(core), cols(j)].astype(F32)
            dp[chip, :, cols(j)] = (mine + dprt[:, cols(j)].astype(F32)).astype(BF16)
            for k in range(1, chips):
                send_target(k, j).start()

        for j in range(PIECES):
            out_piece(0, t_rows, dterm, j)
            mate_target(j).start()
            if j:
                pass_on(j - 1)
        pass_on(PIECES - 1)
        for j in range(PIECES):
            for k in range(1, chips):
                recv_target(k, j).wait_recv()
            delta = dp[0, :, cols(j)].astype(F32)
            for h in range(1, chips):
                delta += dp[h, :, cols(j)].astype(F32)
            yfin[:, cols(j)] = (y_ref[half(core), cols(j)].astype(F32) + delta).astype(BF16)
            shift_target(j, yfin.at[:, cols(j)]).start()
        for j in range(PIECES):
            mate_target(j).wait_send()
            for k in range(1, chips):
                send_target(k, j).wait_send()

    def cross(j, which):
        spot = tland.at[half(which), cols(j)]
        return remote(spot, spot, tf_s.at[j], tf_r.at[j], partner)

    def put_target(j, which, slot):
        return pltpu.make_async_copy(
            tland.at[half(which), cols(j)], to_hbm.at[half(which), cols(j)], o_sem.at[slot, j]
        )

    def put_source(j):
        return pltpu.make_async_copy(sland.at[:, cols(j)], so_hbm.at[:, cols(j)], o_sem.at[2, j])

    for j in range(PIECES):
        shift_target(j, yfin.at[:, cols(j)]).wait_recv()
        cross(j, core).start()
        put_target(j, core, 0).start()
    for j in range(PIECES):
        shift_source(j, fin).wait_recv()
        put_source(j).start()
    for j in range(PIECES):
        cross(j, other).wait_recv()
        put_target(j, other, 1).start()

    to_partner.wait_send()
    for i in range(chunks):
        for k in range(1, chips):
            gather_send(k, i).wait_send()
            forward(k, i, core).wait_send()
    for j in range(PIECES):
        shift_source(j, fin).wait_send()
        shift_target(j, yfin.at[:, cols(j)]).wait_send()
        cross(j, core).wait_send()
        put_target(j, core, 0).wait()
        put_target(j, other, 1).wait()
        put_source(j).wait()


def local(n_sec, n_f, source_rows, target_rows, attn_weights, gains, lengths):
    chips = n_f // 2
    more = max(chips - 1, 1)
    rows, d = source_rows.shape
    t_rows = target_rows.shape[0]
    width = attn_weights.shape[3]
    pair, total, t_half = 2 * rows, rows * n_f, t_rows // 2
    chunks = row_chunks(rows)
    q_rows = max(total, t_rows)
    dma = pltpu.SemaphoreType.DMA
    vmem = lambda *shape: pltpu.VMEM(shape, BF16)
    scratch = [
        vmem(total, d), vmem(pair, d), vmem(t_rows, d), vmem(4, d, width),
        vmem(3, q_rows, width), vmem(q_rows, width),
        vmem(more, pair, d), vmem(more, rows, d), vmem(more, rows, d), vmem(more, rows, d),
        vmem(pair, d), vmem(rows, d), vmem(rows, d), vmem(rows, d),
        vmem(t_rows, d), vmem(t_half, d), vmem(chips, t_half, d), vmem(t_half, d), vmem(t_rows, d),
        dma((4,)), dma, dma((more, chunks)), dma((more, chunks)), dma, dma,
        dma((more, chunks)), dma((more, chunks)),
        dma((more, PIECES)), dma((more, PIECES)), dma((more, PIECES)), dma((more, PIECES)),
        dma((PIECES,)), dma((PIECES,)), dma((PIECES,)), dma((PIECES,)),
        dma((more, PIECES)), dma((more, PIECES)),
        dma((PIECES,)), dma((PIECES,)), dma((PIECES,)), dma((PIECES,)), dma((PIECES,)), dma((PIECES,)),
        dma((3, PIECES)),
    ]
    in_vmem = pl.BlockSpec(memory_space=pltpu.VMEM)
    anywhere = pl.BlockSpec(memory_space=pl.ANY)
    return pl.pallas_call(
        functools.partial(kernel, n_sec, n_f),
        out_shape=(
            jax.ShapeDtypeStruct(source_rows.shape, BF16),
            jax.ShapeDtypeStruct(target_rows.shape, BF16),
        ),
        in_specs=[in_vmem, in_vmem, in_vmem, pl.BlockSpec(memory_space=pltpu.SMEM), anywhere],
        out_specs=(anywhere, anywhere),
        scratch_shapes=scratch,
        compiler_params=pltpu.CompilerParams(
            collective_id=0, has_side_effects=True, vmem_limit_bytes=60 * 1024 * 1024
        ),
    )(source_rows, target_rows, gains, lengths, attn_weights)


def solution(mesh):
    in_specs = (
        P(("section", "fsdp"), None),
        P("section", None),
        P("section", None, None, "fsdp"),
        P("section", None),
        P("section"),
    )
    out_specs = (P(("section", "fsdp"), None), P("section", None))
    body = functools.partial(local, mesh.shape["section"], mesh.shape["fsdp"])
    return jax.shard_map(body, mesh=mesh, in_specs=in_specs, out_specs=out_specs, check_vma=False)
```

```python
import functools

import jax
import jax.numpy as jnp
from jax import lax
from jax.experimental import pallas as pl
from jax.experimental.pallas import tpu as pltpu
from jax.sharding import PartitionSpec as P

HEAD_DIM = 64
PIECES = 8
GATHER = 8
F32 = jnp.float32
BF16 = jnp.bfloat16


def rms_norm(block, gain):
    wide = block.astype(F32)
    inverse = lax.rsqrt(jnp.mean(wide * wide, axis=-1, keepdims=True) + 1e-06)
    return (wide * inverse * gain).astype(BF16)


def kernel(
    n_sec, n_f, x_ref, y_ref, gain_ref, len_ref, w_hbm, so_hbm, to_hbm,
    xs, ny, w, acc, qkv, ctx, term, prt, sums, rem, own, prt_own, fin, sland,
    dterm, dprt, dp, yfin, tland,
    w_sem, ag_s, ag_r, pt_s, pt_r, fw_s, fw_r, t1_s, t1_r, x1_s, x1_r,
    t2_s, t2_r, d1_s, d1_r, d2_s, d2_r, ss_s, ss_r, ts_s, ts_r, tf_s, tf_r, o_sem,
):
    chips = n_f // 2
    rows, d = x_ref.shape
    pair = 2 * rows
    total = pair * chips
    t_rows = y_ref.shape[0]
    t_half = t_rows // 2
    width = w.shape[2]
    cn, gn = d // PIECES, d // GATHER
    sec, f = lax.axis_index("section"), lax.axis_index("fsdp")
    core, chip = lax.rem(f, 2), f // 2
    other = 1 - core
    enc = sec < n_sec // 2
    partner = {"fsdp": chip * 2 + other}
    nxt = {"section": lax.rem(sec + 1, n_sec)}
    prv = {"section": lax.rem(sec + n_sec - 1, n_sec)}

    def ahead(k):
        return lax.rem(chip + k, chips)

    def behind(k):
        return lax.rem(chip + chips - k, chips)

    def peer(h):
        return {"fsdp": h * 2 + core}

    def remote(src, dst, send, recv, dev):
        return pltpu.make_async_remote_copy(
            src_ref=src, dst_ref=dst, send_sem=send, recv_sem=recv,
            device_id=dev, device_id_type=pl.DeviceIdType.MESH,
        )

    def at(start, size):
        return pl.ds(pl.multiple_of(start, 16), size)

    def cols(j):
        return pl.ds(j * cn, cn)

    barrier = pltpu.get_barrier_semaphore()
    greet = [partner, nxt, prv] + [peer(ahead(k)) for k in range(1, chips)]
    for dev in greet:
        pl.semaphore_signal(barrier, inc=1, device_id=dev, device_id_type=pl.DeviceIdType.MESH)

    w_copies = [pltpu.make_async_copy(w_hbm.at[0, i], w.at[i], w_sem.at[i]) for i in range(4)]
    for cp in w_copies:
        cp.start()
    gain = gain_ref[...]

    def norm_rows(src, dst, dst_start, count):
        size = 32 if count % 32 == 0 else 16

        def step(r, carry):
            dst[at(dst_start + r * size, size), :] = rms_norm(src[at(r * size, size), :], gain)
            return carry

        lax.fori_loop(0, count // size, step, 0)

    @pl.when(enc)
    def _():
        norm_rows(x_ref, xs, f * rows, rows)

    @pl.when(jnp.logical_not(enc))
    def _():
        xs[at(f * rows, rows), :] = x_ref[...]

    pl.semaphore_wait(barrier, len(greet))

    def block(h, which):
        return at((h * 2 + which) * rows, rows)

    def gather_send(k, j):
        spot = xs.at[block(chip, core), pl.ds(j * gn, gn)]
        return remote(spot, spot, ag_s.at[k - 1, j], ag_r.at[k - 1, j], peer(ahead(k)))

    def gather_recv(k, j):
        spot = xs.at[block(behind(k), core), pl.ds(j * gn, gn)]
        return remote(spot, spot, ag_s.at[k - 1, j], ag_r.at[k - 1, j], peer(behind(k)))

    def forward(k, j, which):
        spot = xs.at[block(behind(k), which), pl.ds(j * gn, gn)]
        return remote(spot, spot, fw_s.at[k - 1, j], fw_r.at[k - 1, j], partner)

    def swap(which):
        spot = xs.at[block(chip, which), :]
        return remote(spot, spot, pt_s, pt_r, partner)

    for j in range(GATHER):
        for k in range(1, chips):
            gather_send(k, j).start()
    swap(core).start()

    def shift_source(j, src):
        return remote(src.at[:, cols(j)], sland.at[:, cols(j)], ss_s.at[j], ss_r.at[j], nxt)

    def half(which):
        return at(which * t_half, t_half)

    def shift_target(j, src):
        return remote(src, tland.at[half(core), cols(j)], ts_s.at[j], ts_r.at[j], nxt)

    @pl.when(enc)
    def _():
        for j in range(PIECES):
            shift_target(j, y_ref.at[half(core), cols(j)]).start()

    @pl.when(jnp.logical_not(enc))
    def _():
        for j in range(PIECES):
            shift_source(j, x_ref).start()

    def project(src, which, start, count):
        qkv[which, at(start, count), :] = jnp.dot(
            src, w[which], preferred_element_type=F32
        ).astype(BF16)

    def project_piece(which, h, j):
        part = jnp.dot(
            xs[at(h * pair, pair), pl.ds(j * gn, gn)], w[which, pl.ds(j * gn, gn), :],
            preferred_element_type=F32,
        )
        if j:
            part = part + acc[which]
        if j < GATHER - 1:
            acc[which] = part
        else:
            qkv[which, at(h * pair, pair), :] = part.astype(BF16)

    @pl.when(jnp.logical_not(enc))
    def _():
        norm_rows(y_ref, ny, 0, t_rows)

    w_copies[0].wait()

    @pl.when(jnp.logical_not(enc))
    def _():
        project(ny[...], 0, 0, t_rows)

    swap(other).wait_recv()

    @pl.when(enc)
    def _():
        project(xs[at(chip * pair, pair), :], 0, chip * pair, pair)

    for which in (1, 2):
        w_copies[which].wait()
        project(xs[at(chip * pair, pair), :], which, chip * pair, pair)

    for k in range(1, chips):
        for j in range(GATHER):
            gather_recv(k, j).wait_recv()
            forward(k, j, core).start()
            forward(k, j, other).wait_recv()

            @pl.when(enc)
            def _():
                project_piece(0, behind(k), j)

            project_piece(1, behind(k), j)
            project_piece(2, behind(k), j)

    length = len_ref[0]

    def attend(start, count):
        key_ok = lax.broadcasted_iota(jnp.int32, (1, total), 1) < length
        first = lax.broadcasted_iota(jnp.int32, (1, 2 * HEAD_DIM), 1) < HEAD_DIM

        def step(t, carry):
            lanes = pl.ds(pl.multiple_of(t * 2 * HEAD_DIM, 128), 2 * HEAD_DIM)
            queries = qkv[0, at(start, count), lanes]
            keys, values = qkv[1, :total, lanes], qkv[2, :total, lanes]
            low = queries * jnp.where(first, 0.125, 0.0).astype(BF16)
            high = queries * jnp.where(first, 0.0, 0.125).astype(BF16)
            scores = lax.dot_general(
                jnp.concatenate([low, high], axis=0), keys, (((1,), (1,)), ((), ())),
                preferred_element_type=F32,
            )
            scores = jnp.where(key_ok, scores, -1000000000.0)
            expo = jnp.exp(scores - jnp.max(scores, axis=-1, keepdims=True))
            soft = (expo * (1.0 / jnp.sum(expo, axis=-1, keepdims=True))).astype(BF16)
            mixed = jnp.dot(soft, values, preferred_element_type=F32)
            ctx[at(start, count), lanes] = jnp.where(
                first, mixed[:count], mixed[count:]
            ).astype(BF16)
            return carry

        lax.fori_loop(0, width // (2 * HEAD_DIM), step, 0)

    on = min(cn, 1024)

    def out_piece(start, count, dst, j):
        def step(t, carry):
            lanes = pl.ds(pl.multiple_of(j * cn + t * on, 128), on)
            dst[:, lanes] = lax.dot_general(
                ctx[at(start, count), :], w[3, lanes, :], (((1,), (1,)), ((), ())),
                preferred_element_type=F32,
            ).astype(BF16)
            return carry

        lax.fori_loop(0, cn // on, step, 0)

    def mate_term(k, j):
        return remote(
            term.at[k - 1, at(other * rows, rows), cols(j)], prt.at[k - 1, :, cols(j)],
            t1_s.at[k - 1, j], t1_r.at[k - 1, j], partner,
        )

    def send_sum(k, j):
        return remote(
            sums.at[k - 1, :, cols(j)], rem.at[k - 1, :, cols(j)],
            x1_s.at[k - 1, j], x1_r.at[k - 1, j], peer(ahead(k)),
        )

    def mate_own(j):
        return remote(
            own.at[at(other * rows, rows), cols(j)], prt_own.at[:, cols(j)],
            t2_s.at[j], t2_r.at[j], partner,
        )

    def mate_target(j):
        return remote(
            dterm.at[half(other), cols(j)], dprt.at[:, cols(j)], d1_s.at[j], d1_r.at[j], partner
        )

    def send_target(k, j):
        return remote(
            dp.at[chip, :, cols(j)], dp.at[chip, :, cols(j)],
            d2_s.at[k - 1, j], d2_r.at[k - 1, j], peer(ahead(k)),
        )

    def recv_target(k, j):
        spot = dp.at[behind(k), :, cols(j)]
        return remote(spot, spot, d2_s.at[k - 1, j], d2_r.at[k - 1, j], peer(behind(k)))

    w_copies[3].wait()

    @pl.when(enc)
    def _():
        for k in range(1, chips):
            start = ahead(k) * pair
            attend(start, pair)

            def pass_on(j):
                mate_term(k, j).wait_recv()
                mine = term[k - 1, at(core * rows, rows), cols(j)].astype(F32)
                sums[k - 1, :, cols(j)] = (mine + prt[k - 1, :, cols(j)].astype(F32)).astype(BF16)
                send_sum(k, j).start()

            for j in range(PIECES):
                out_piece(start, pair, term.at[k - 1], j)
                mate_term(k, j).start()
                if j:
                    pass_on(j - 1)
            pass_on(PIECES - 1)
        attend(chip * pair, pair)
        for j in range(PIECES):
            out_piece(chip * pair, pair, own, j)
            mate_own(j).start()
        for j in range(PIECES):
            mate_own(j).wait_recv()
            delta = own[at(core * rows, rows), cols(j)].astype(F32) + prt_own[:, cols(j)].astype(F32)
            for k in range(1, chips):
                send_sum(k, j).wait_recv()
                delta += rem[k - 1, :, cols(j)].astype(F32)
            fin[:, cols(j)] = (x_ref[:, cols(j)].astype(F32) + delta).astype(BF16)
            shift_source(j, fin).start()
        for j in range(PIECES):
            mate_own(j).wait_send()
            for k in range(1, chips):
                mate_term(k, j).wait_send()
                send_sum(k, j).wait_send()

    @pl.when(jnp.logical_not(enc))
    def _():
        attend(0, t_rows)

        def pass_on(j):
            mate_target(j).wait_recv()
            mine = dterm[half(core), cols(j)].astype(F32)
            dp[chip, :, cols(j)] = (mine + dprt[:, cols(j)].astype(F32)).astype(BF16)
            for k in range(1, chips):
                send_target(k, j).start()

        for j in range(PIECES):
            out_piece(0, t_rows, dterm, j)
            mate_target(j).start()
            if j:
                pass_on(j - 1)
        pass_on(PIECES - 1)
        for j in range(PIECES):
            for k in range(1, chips):
                recv_target(k, j).wait_recv()
            delta = dp[0, :, cols(j)].astype(F32)
            for h in range(1, chips):
                delta += dp[h, :, cols(j)].astype(F32)
            yfin[:, cols(j)] = (y_ref[half(core), cols(j)].astype(F32) + delta).astype(BF16)
            shift_target(j, yfin.at[:, cols(j)]).start()
        for j in range(PIECES):
            mate_target(j).wait_send()
            for k in range(1, chips):
                send_target(k, j).wait_send()

    def cross(j, which):
        spot = tland.at[half(which), cols(j)]
        return remote(spot, spot, tf_s.at[j], tf_r.at[j], partner)

    def put_target(j, which, slot):
        return pltpu.make_async_copy(
            tland.at[half(which), cols(j)], to_hbm.at[half(which), cols(j)], o_sem.at[slot, j]
        )

    def put_source(j):
        return pltpu.make_async_copy(sland.at[:, cols(j)], so_hbm.at[:, cols(j)], o_sem.at[2, j])

    for j in range(PIECES):
        shift_target(j, yfin.at[:, cols(j)]).wait_recv()
        cross(j, core).start()
        put_target(j, core, 0).start()
    for j in range(PIECES):
        shift_source(j, fin).wait_recv()
        put_source(j).start()
    for j in range(PIECES):
        cross(j, other).wait_recv()
        put_target(j, other, 1).start()

    swap(core).wait_send()
    for j in range(GATHER):
        for k in range(1, chips):
            gather_send(k, j).wait_send()
            forward(k, j, core).wait_send()
    for j in range(PIECES):
        shift_source(j, fin).wait_send()
        shift_target(j, yfin.at[:, cols(j)]).wait_send()
        cross(j, core).wait_send()
        put_target(j, core, 0).wait()
        put_target(j, other, 1).wait()
        put_source(j).wait()


def local(n_sec, n_f, source_rows, target_rows, attn_weights, gains, lengths):
    chips = n_f // 2
    more = max(chips - 1, 1)
    rows, d = source_rows.shape
    t_rows = target_rows.shape[0]
    width = attn_weights.shape[3]
    pair, total, t_half = 2 * rows, rows * n_f, t_rows // 2
    q_rows = max(total, t_rows)
    dma = pltpu.SemaphoreType.DMA
    vmem = lambda *shape: pltpu.VMEM(shape, BF16)
    scratch = [
        vmem(total, d), vmem(t_rows, d), vmem(4, d, width), pltpu.VMEM((3, pair, width), F32),
        vmem(3, q_rows, width), vmem(q_rows, width),
        vmem(more, pair, d), vmem(more, rows, d), vmem(more, rows, d), vmem(more, rows, d),
        vmem(pair, d), vmem(rows, d), vmem(rows, d), vmem(rows, d),
        vmem(t_rows, d), vmem(t_half, d), vmem(chips, t_half, d), vmem(t_half, d), vmem(t_rows, d),
        dma((4,)), dma((more, GATHER)), dma((more, GATHER)), dma, dma,
        dma((more, GATHER)), dma((more, GATHER)),
        dma((more, PIECES)), dma((more, PIECES)), dma((more, PIECES)), dma((more, PIECES)),
        dma((PIECES,)), dma((PIECES,)), dma((PIECES,)), dma((PIECES,)),
        dma((more, PIECES)), dma((more, PIECES)),
        dma((PIECES,)), dma((PIECES,)), dma((PIECES,)), dma((PIECES,)), dma((PIECES,)), dma((PIECES,)),
        dma((3, PIECES)),
    ]
    in_vmem = pl.BlockSpec(memory_space=pltpu.VMEM)
    anywhere = pl.BlockSpec(memory_space=pl.ANY)
    return pl.pallas_call(
        functools.partial(kernel, n_sec, n_f),
        out_shape=(
            jax.ShapeDtypeStruct(source_rows.shape, BF16),
            jax.ShapeDtypeStruct(target_rows.shape, BF16),
        ),
        in_specs=[in_vmem, in_vmem, in_vmem, pl.BlockSpec(memory_space=pltpu.SMEM), anywhere],
        out_specs=(anywhere, anywhere),
        scratch_shapes=scratch,
        compiler_params=pltpu.CompilerParams(
            collective_id=0, has_side_effects=True, vmem_limit_bytes=60 * 1024 * 1024
        ),
    )(source_rows, target_rows, gains, lengths, attn_weights)


def solution(mesh):
    in_specs = (
        P(("section", "fsdp"), None),
        P("section", None),
        P("section", None, None, "fsdp"),
        P("section", None),
        P("section"),
    )
    out_specs = (P(("section", "fsdp"), None), P("section", None))
    body = functools.partial(local, mesh.shape["section"], mesh.shape["fsdp"])
    return jax.shard_map(body, mesh=mesh, in_specs=in_specs, out_specs=out_specs, check_vma=False)
```

```python
import functools

import jax
import jax.numpy as jnp
from jax import lax
from jax.experimental import pallas as pl
from jax.experimental.pallas import tpu as pltpu
from jax.sharding import PartitionSpec as P

HEAD_DIM = 64
PIECES = 4
GATHER = 4
F32 = jnp.float32
BF16 = jnp.bfloat16


def rms_norm(block, gain):
    wide = block.astype(F32)
    inverse = lax.rsqrt(jnp.mean(wide * wide, axis=-1, keepdims=True) + 1e-06)
    return (wide * inverse * gain).astype(BF16)


def kernel(
    n_sec, n_f, x_ref, y_ref, gain_ref, len_ref, w_hbm, so_hbm, to_hbm,
    xs, ny, w, acc, qkv, ctx, term, prt, sums, rem, own, prt_own, fin, sland,
    dterm, dprt, dp, yfin, tland,
    w_sem, ag_s, ag_r, pt_s, pt_r, fw_s, fw_r, t1_s, t1_r, x1_s, x1_r,
    t2_s, t2_r, d1_s, d1_r, d2_s, d2_r, ss_s, ss_r, ts_s, ts_r, tf_s, tf_r, o_sem,
):
    chips = n_f // 2
    rows, d = x_ref.shape
    pair = 2 * rows
    total = pair * chips
    t_rows = y_ref.shape[0]
    t_half = t_rows // 2
    width = w.shape[2]
    cn, gn = d // PIECES, d // GATHER
    sec, f = lax.axis_index("section"), lax.axis_index("fsdp")
    core, chip = lax.rem(f, 2), f // 2
    other = 1 - core
    enc = sec < n_sec // 2
    partner = {"fsdp": chip * 2 + other}
    nxt = {"section": lax.rem(sec + 1, n_sec)}
    prv = {"section": lax.rem(sec + n_sec - 1, n_sec)}

    def ahead(k):
        return lax.rem(chip + k, chips)

    def behind(k):
        return lax.rem(chip + chips - k, chips)

    def peer(h):
        return {"fsdp": h * 2 + core}

    def remote(src, dst, send, recv, dev):
        return pltpu.make_async_remote_copy(
            src_ref=src, dst_ref=dst, send_sem=send, recv_sem=recv,
            device_id=dev, device_id_type=pl.DeviceIdType.MESH,
        )

    def at(start, size):
        return pl.ds(pl.multiple_of(start, 16), size)

    def cols(j):
        return pl.ds(j * cn, cn)

    barrier = pltpu.get_barrier_semaphore()
    greet = [partner, nxt, prv] + [peer(ahead(k)) for k in range(1, chips)]
    for dev in greet:
        pl.semaphore_signal(barrier, inc=1, device_id=dev, device_id_type=pl.DeviceIdType.MESH)

    w_copies = [pltpu.make_async_copy(w_hbm.at[0, i], w.at[i], w_sem.at[i]) for i in range(4)]
    for cp in w_copies:
        cp.start()
    gain = gain_ref[...]

    def norm_rows(src, dst, dst_start, count):
        size = 32 if count % 32 == 0 else 16

        def step(r, carry):
            dst[at(dst_start + r * size, size), :] = rms_norm(src[at(r * size, size), :], gain)
            return carry

        lax.fori_loop(0, count // size, step, 0)

    @pl.when(enc)
    def _():
        norm_rows(x_ref, xs, f * rows, rows)

    @pl.when(jnp.logical_not(enc))
    def _():
        xs[at(f * rows, rows), :] = x_ref[...]

    pl.semaphore_wait(barrier, len(greet))

    def block(h, which):
        return at((h * 2 + which) * rows, rows)

    def gather_send(k, j):
        spot = xs.at[block(chip, core), pl.ds(j * gn, gn)]
        return remote(spot, spot, ag_s.at[k - 1, j], ag_r.at[k - 1, j], peer(ahead(k)))

    def gather_recv(k, j):
        spot = xs.at[block(behind(k), core), pl.ds(j * gn, gn)]
        return remote(spot, spot, ag_s.at[k - 1, j], ag_r.at[k - 1, j], peer(behind(k)))

    def forward(k, j, which):
        spot = xs.at[block(behind(k), which), pl.ds(j * gn, gn)]
        return remote(spot, spot, fw_s.at[k - 1, j], fw_r.at[k - 1, j], partner)

    def swap(which):
        spot = xs.at[block(chip, which), :]
        return remote(spot, spot, pt_s, pt_r, partner)

    for j in range(GATHER):
        for k in range(1, chips):
            gather_send(k, j).start()
    swap(core).start()

    def shift_source(j, src):
        return remote(src.at[:, cols(j)], sland.at[:, cols(j)], ss_s.at[j], ss_r.at[j], nxt)

    def half(which):
        return at(which * t_half, t_half)

    def shift_target(j, src):
        return remote(src, tland.at[half(core), cols(j)], ts_s.at[j], ts_r.at[j], nxt)

    @pl.when(enc)
    def _():
        for j in range(PIECES):
            shift_target(j, y_ref.at[half(core), cols(j)]).start()

    @pl.when(jnp.logical_not(enc))
    def _():
        for j in range(PIECES):
            shift_source(j, x_ref).start()

    def project(src, which, start, count):
        qkv[which, at(start, count), :] = jnp.dot(
            src, w[which], preferred_element_type=F32
        ).astype(BF16)

    def project_piece(which, h, j):
        part = jnp.dot(
            xs[at(h * pair, pair), pl.ds(j * gn, gn)], w[which, pl.ds(j * gn, gn), :],
            preferred_element_type=F32,
        )
        if j:
            part = part + acc[which]
        if j < GATHER - 1:
            acc[which] = part
        else:
            qkv[which, at(h * pair, pair), :] = part.astype(BF16)

    @pl.when(jnp.logical_not(enc))
    def _():
        norm_rows(y_ref, ny, 0, t_rows)

    w_copies[0].wait()

    @pl.when(jnp.logical_not(enc))
    def _():
        project(ny[...], 0, 0, t_rows)

    swap(other).wait_recv()

    @pl.when(enc)
    def _():
        project(xs[at(chip * pair, pair), :], 0, chip * pair, pair)

    for which in (1, 2):
        w_copies[which].wait()
        project(xs[at(chip * pair, pair), :], which, chip * pair, pair)

    for k in range(1, chips):
        for j in range(GATHER):
            gather_recv(k, j).wait_recv()
            forward(k, j, core).start()
            forward(k, j, other).wait_recv()

            @pl.when(enc)
            def _():
                project_piece(0, behind(k), j)

            project_piece(1, behind(k), j)
            project_piece(2, behind(k), j)

    length = len_ref[0]

    def attend(start, count):
        key_ok = lax.broadcasted_iota(jnp.int32, (1, total), 1) < length
        first = lax.broadcasted_iota(jnp.int32, (1, 2 * HEAD_DIM), 1) < HEAD_DIM

        def step(t, carry):
            lanes = pl.ds(pl.multiple_of(t * 2 * HEAD_DIM, 128), 2 * HEAD_DIM)
            queries = qkv[0, at(start, count), lanes]
            keys, values = qkv[1, :total, lanes], qkv[2, :total, lanes]
            low = queries * jnp.where(first, 0.125, 0.0).astype(BF16)
            high = queries * jnp.where(first, 0.0, 0.125).astype(BF16)
            scores = lax.dot_general(
                jnp.concatenate([low, high], axis=0), keys, (((1,), (1,)), ((), ())),
                preferred_element_type=F32,
            )
            scores = jnp.where(key_ok, scores, -1000000000.0)
            expo = jnp.exp(scores - jnp.max(scores, axis=-1, keepdims=True))
            soft = (expo * (1.0 / jnp.sum(expo, axis=-1, keepdims=True))).astype(BF16)
            mixed = jnp.dot(soft, values, preferred_element_type=F32)
            ctx[at(start, count), lanes] = jnp.where(
                first, mixed[:count], mixed[count:]
            ).astype(BF16)
            return carry

        lax.fori_loop(0, width // (2 * HEAD_DIM), step, 0)

    on = min(cn, 1024)

    def out_piece(start, count, dst, j):
        def step(t, carry):
            lanes = pl.ds(pl.multiple_of(j * cn + t * on, 128), on)
            dst[:, lanes] = lax.dot_general(
                ctx[at(start, count), :], w[3, lanes, :], (((1,), (1,)), ((), ())),
                preferred_element_type=F32,
            ).astype(BF16)
            return carry

        lax.fori_loop(0, cn // on, step, 0)

    def mate_term(k, j):
        return remote(
            term.at[k - 1, at(other * rows, rows), cols(j)], prt.at[k - 1, :, cols(j)],
            t1_s.at[k - 1, j], t1_r.at[k - 1, j], partner,
        )

    def send_sum(k, j):
        return remote(
            sums.at[k - 1, :, cols(j)], rem.at[k - 1, :, cols(j)],
            x1_s.at[k - 1, j], x1_r.at[k - 1, j], peer(ahead(k)),
        )

    def mate_own(j):
        return remote(
            own.at[at(other * rows, rows), cols(j)], prt_own.at[:, cols(j)],
            t2_s.at[j], t2_r.at[j], partner,
        )

    def mate_target(j):
        return remote(
            dterm.at[half(other), cols(j)], dprt.at[:, cols(j)], d1_s.at[j], d1_r.at[j], partner
        )

    def send_target(k, j):
        return remote(
            dp.at[chip, :, cols(j)], dp.at[chip, :, cols(j)],
            d2_s.at[k - 1, j], d2_r.at[k - 1, j], peer(ahead(k)),
        )

    def recv_target(k, j):
        spot = dp.at[behind(k), :, cols(j)]
        return remote(spot, spot, d2_s.at[k - 1, j], d2_r.at[k - 1, j], peer(behind(k)))

    w_copies[3].wait()

    @pl.when(enc)
    def _():
        for k in range(1, chips):
            start = ahead(k) * pair
            attend(start, pair)

            def pass_on(j):
                mate_term(k, j).wait_recv()
                mine = term[k - 1, at(core * rows, rows), cols(j)].astype(F32)
                sums[k - 1, :, cols(j)] = (mine + prt[k - 1, :, cols(j)].astype(F32)).astype(BF16)
                send_sum(k, j).start()

            for j in range(PIECES):
                out_piece(start, pair, term.at[k - 1], j)
                mate_term(k, j).start()
                if j:
                    pass_on(j - 1)
            pass_on(PIECES - 1)
        attend(chip * pair, pair)
        for j in range(PIECES):
            out_piece(chip * pair, pair, own, j)
            mate_own(j).start()
        for j in range(PIECES):
            mate_own(j).wait_recv()
            delta = own[at(core * rows, rows), cols(j)].astype(F32) + prt_own[:, cols(j)].astype(F32)
            for k in range(1, chips):
                send_sum(k, j).wait_recv()
                delta += rem[k - 1, :, cols(j)].astype(F32)
            fin[:, cols(j)] = (x_ref[:, cols(j)].astype(F32) + delta).astype(BF16)
            shift_source(j, fin).start()
        for j in range(PIECES):
            mate_own(j).wait_send()
            for k in range(1, chips):
                mate_term(k, j).wait_send()
                send_sum(k, j).wait_send()

    @pl.when(jnp.logical_not(enc))
    def _():
        attend(0, t_rows)

        def pass_on(j):
            mate_target(j).wait_recv()
            mine = dterm[half(core), cols(j)].astype(F32)
            dp[chip, :, cols(j)] = (mine + dprt[:, cols(j)].astype(F32)).astype(BF16)
            for k in range(1, chips):
                send_target(k, j).start()

        for j in range(PIECES):
            out_piece(0, t_rows, dterm, j)
            mate_target(j).start()
            if j:
                pass_on(j - 1)
        pass_on(PIECES - 1)
        for j in range(PIECES):
            for k in range(1, chips):
                recv_target(k, j).wait_recv()
            delta = dp[0, :, cols(j)].astype(F32)
            for h in range(1, chips):
                delta += dp[h, :, cols(j)].astype(F32)
            yfin[:, cols(j)] = (y_ref[half(core), cols(j)].astype(F32) + delta).astype(BF16)
            shift_target(j, yfin.at[:, cols(j)]).start()
        for j in range(PIECES):
            mate_target(j).wait_send()
            for k in range(1, chips):
                send_target(k, j).wait_send()

    def cross(j, which):
        spot = tland.at[half(which), cols(j)]
        return remote(spot, spot, tf_s.at[j], tf_r.at[j], partner)

    def put_target(j, which, slot):
        return pltpu.make_async_copy(
            tland.at[half(which), cols(j)], to_hbm.at[half(which), cols(j)], o_sem.at[slot, j]
        )

    def put_source(j):
        return pltpu.make_async_copy(sland.at[:, cols(j)], so_hbm.at[:, cols(j)], o_sem.at[2, j])

    for j in range(PIECES):
        shift_target(j, yfin.at[:, cols(j)]).wait_recv()
        cross(j, core).start()
        put_target(j, core, 0).start()
    for j in range(PIECES):
        shift_source(j, fin).wait_recv()
        put_source(j).start()
    for j in range(PIECES):
        cross(j, other).wait_recv()
        put_target(j, other, 1).start()

    swap(core).wait_send()
    for j in range(GATHER):
        for k in range(1, chips):
            gather_send(k, j).wait_send()
            forward(k, j, core).wait_send()
    for j in range(PIECES):
        shift_source(j, fin).wait_send()
        shift_target(j, yfin.at[:, cols(j)]).wait_send()
        cross(j, core).wait_send()
        put_target(j, core, 0).wait()
        put_target(j, other, 1).wait()
        put_source(j).wait()


def local(n_sec, n_f, source_rows, target_rows, attn_weights, gains, lengths):
    chips = n_f // 2
    more = max(chips - 1, 1)
    rows, d = source_rows.shape
    t_rows = target_rows.shape[0]
    width = attn_weights.shape[3]
    pair, total, t_half = 2 * rows, rows * n_f, t_rows // 2
    q_rows = max(total, t_rows)
    dma = pltpu.SemaphoreType.DMA
    vmem = lambda *shape: pltpu.VMEM(shape, BF16)
    scratch = [
        vmem(total, d), vmem(t_rows, d), vmem(4, d, width), pltpu.VMEM((3, pair, width), F32),
        vmem(3, q_rows, width), vmem(q_rows, width),
        vmem(more, pair, d), vmem(more, rows, d), vmem(more, rows, d), vmem(more, rows, d),
        vmem(pair, d), vmem(rows, d), vmem(rows, d), vmem(rows, d),
        vmem(t_rows, d), vmem(t_half, d), vmem(chips, t_half, d), vmem(t_half, d), vmem(t_rows, d),
        dma((4,)), dma((more, GATHER)), dma((more, GATHER)), dma, dma,
        dma((more, GATHER)), dma((more, GATHER)),
        dma((more, PIECES)), dma((more, PIECES)), dma((more, PIECES)), dma((more, PIECES)),
        dma((PIECES,)), dma((PIECES,)), dma((PIECES,)), dma((PIECES,)),
        dma((more, PIECES)), dma((more, PIECES)),
        dma((PIECES,)), dma((PIECES,)), dma((PIECES,)), dma((PIECES,)), dma((PIECES,)), dma((PIECES,)),
        dma((3, PIECES)),
    ]
    in_vmem = pl.BlockSpec(memory_space=pltpu.VMEM)
    anywhere = pl.BlockSpec(memory_space=pl.ANY)
    moved = pl.pallas_call(
        functools.partial(kernel, n_sec, n_f),
        out_shape=(
            pltpu.VMEM(source_rows.shape, BF16),
            pltpu.VMEM(target_rows.shape, BF16),
        ),
        in_specs=[in_vmem, in_vmem, in_vmem, pl.BlockSpec(memory_space=pltpu.SMEM), anywhere],
        out_specs=(anywhere, anywhere),
        scratch_shapes=scratch,
        compiler_params=pltpu.CompilerParams(
            collective_id=0, has_side_effects=True, vmem_limit_bytes=52 * 1024 * 1024
        ),
    )(source_rows, target_rows, gains, lengths, attn_weights)
    return settle(*moved)


def settle(source, target):
    def body(a_ref, b_ref, a_out, b_out, a_vmem, b_vmem, in_sem, out_sem):
        plan = []
        for src, mid, dst in ((a_ref, a_vmem, a_out), (b_ref, b_vmem, b_out)):
            step = src.shape[1] // 4
            for j in range(4):
                lanes = pl.ds(j * step, step)
                n = len(plan)
                plan.append((
                    pltpu.make_async_copy(src.at[:, lanes], mid.at[:, lanes], in_sem.at[n]),
                    pltpu.make_async_copy(mid.at[:, lanes], dst.at[:, lanes], out_sem.at[n]),
                ))
        for into, _ in plan:
            into.start()
        for into, out in plan:
            into.wait()
            out.start()
        for _, out in plan:
            out.wait()

    anywhere = pl.BlockSpec(memory_space=pl.ANY)
    return pl.pallas_call(
        body,
        out_shape=tuple(jax.ShapeDtypeStruct(v.shape, v.dtype) for v in (source, target)),
        in_specs=[anywhere, anywhere],
        out_specs=(anywhere, anywhere),
        scratch_shapes=[
            pltpu.VMEM(source.shape, source.dtype), pltpu.VMEM(target.shape, target.dtype),
            pltpu.SemaphoreType.DMA((8,)), pltpu.SemaphoreType.DMA((8,)),
        ],
        compiler_params=pltpu.CompilerParams(vmem_limit_bytes=8 * 1024 * 1024),
    )(source, target)


def solution(mesh):
    in_specs = (
        P(("section", "fsdp"), None),
        P("section", None),
        P("section", None, None, "fsdp"),
        P("section", None),
        P("section"),
    )
    out_specs = (P(("section", "fsdp"), None), P("section", None))
    body = functools.partial(local, mesh.shape["section"], mesh.shape["fsdp"])
    return jax.shard_map(body, mesh=mesh, in_specs=in_specs, out_specs=out_specs, check_vma=False)
```
